512 devices in a mesh: parts: 2 (over y), brick: 16 (over z), rep: 8 (over x), sub: 2 (over core).
Axes of the slice: x: 8, y: 2, z: 16, core: 2. Of those that a mesh axis runs over, the one named last changes fastest.
The devices are a block of a 8x8x16 slice.
Arguments:
- fine_cells: int32 [5, 524288], P(None, ('parts', 'brick', 'rep', 'sub')), parts along dimension 1, may hold values from 0 to 511, as said below
- fine_exponent: float32 [524288], P(('parts', 'brick', 'rep', 'sub')), parts along dimension 0, may hold values from 0.05 to 0.6
- fine_charge: float32 [524288], P(('parts', 'brick', 'rep', 'sub')), parts along dimension 0, may hold values from -6 to 6
- fine_offset: float32 [3, 524288], P(None, ('parts', 'brick', 'rep', 'sub')), parts along dimension 1, may hold values from 0 to 1
- wide_cells: int32 [5, 65536], P(None, ('parts', 'brick', 'rep', 'sub')), parts along dimension 1, may hold values from 0 to 127, as said below
- wide_exponent: float32 [65536], P(('parts', 'brick', 'rep', 'sub')), parts along dimension 0, may hold values from 0.05 to 0.6
- wide_charge: float32 [65536], P(('parts', 'brick', 'rep', 'sub')), parts along dimension 0, may hold values from -6 to 6
- wide_offset: float32 [3, 65536], P(None, ('parts', 'brick', 'rep', 'sub')), parts along dimension 1, may hold values from 0 to 1
Outputs:
- finest_grid: float32 [256, 512, 512], P(('parts', 'brick'), ('rep', 'sub')), parts along dimension 0
- second_grid: float32 [128, 256, 256], P(('parts', 'brick'), ('rep', 'sub')), parts along dimension 0
- middle_grid: float32 [64, 16384], P('parts', 'brick'), parts along dimension 0
- coarse_grid: float32 [32, 4096], P('parts', 'brick'), parts along dimension 0
- coarsest_grid: float32 [16, 1024], P('parts', 'brick'), parts along dimension 0
The draws below stay inside these ranges and needn't reach their ends.
There are 2 independent parts, one for each index of `parts`. The reference program is written for one: setup_inputs(seed, part) draws one part's arguments, and reference() takes and returns one part's arrays. A program takes and returns all parts, laid end to end along the dimension named above; each array names one. Nothing has to cross between parts.
Inputs may be any that keep to these rules, and one draw needn't show every extreme that they name: `fine_cells`: column n is one fine Gaussian: row 0 its level L (0 or 1), row 1 its radius (1 to 4, equal to 4 on every 16th column), rows 2 to 4 its centre cell on level L's grid. The centre lies in the block of the device that holds column n: along the first dimension within that device's brick block of 128/2^L/16 cells, along the second within its block of 512/2^L/16 cells along rep+sub, anywhere along the third. `wide_cells`: column n is one wide Gaussian: row 0 its level L (2 to 4), row 1 its radius (1 to 4, equal to 4 on every 16th column), rows 2 to 4 its centre cell, anywhere on level L's grid.
All inputs are finite; a program needn't handle non-finite values.
Results may differ from the reference program's by a relative error of at most 0.0038.
Values sent between devices are 32-bit elements; how exact they have to be, the bound alone decides.
A program may use at most 64 MiB of HBM per device.

```python
import math
import jax
import jax.numpy as jnp
from jax import lax

GRID = 512
ROWS = 128
HALF = 4
FINE_DEV = 1024
WIDE_DEV = 128
FINE = 262144
WIDE = 32768
N_BRICK = 16
N_REP = 8
N_SUB = 2


def draw_fine_cells(key, part):
    slot_count = FINE_DEV * N_BRICK * N_REP * N_SUB
    slots = jnp.arange(slot_count, dtype=jnp.int32)
    device = slots // FINE_DEV
    columns = N_REP * N_SUB
    brick_index = device // columns
    column_index = device % columns
    level_row = (jax.random.randint(jax.random.fold_in(key, 1), (slot_count,), 0, 4) == 0).astype(jnp.int32)
    radius = jax.random.randint(jax.random.fold_in(key, 2), (slot_count,), 1, HALF + 1)
    radius = jnp.where(slots % 16 == 0, HALF, radius)
    row_tile = jnp.right_shift(jnp.int32(ROWS), level_row) // N_BRICK
    period = jnp.right_shift(jnp.int32(GRID), level_row)
    col_tile = period // columns
    picks = jax.random.randint(jax.random.fold_in(key, 3), (3, slot_count), 0, 1 << 20)
    first_cell = brick_index * row_tile + picks[0] % row_tile
    second_cell = column_index * col_tile + picks[1] % col_tile
    third_cell = picks[2] % period
    return jnp.stack([level_row, radius, first_cell, second_cell, third_cell]).astype(jnp.int32)


def draw_wide_cells(key, part):
    slot_count = WIDE_DEV * N_BRICK * N_REP * N_SUB
    slots = jnp.arange(slot_count, dtype=jnp.int32)
    choose = jax.random.randint(jax.random.fold_in(key, 5), (slot_count,), 0, 8)
    level_row = jnp.where(slots % 8 == 3, 4, jnp.where(choose < 2, 3, 2)).astype(jnp.int32)
    radius = jax.random.randint(jax.random.fold_in(key, 6), (slot_count,), 1, HALF + 1)
    radius = jnp.where(slots % 16 == 0, HALF, radius)
    rows_here = jnp.right_shift(jnp.int32(ROWS), level_row)
    period = jnp.right_shift(jnp.int32(GRID), level_row)
    picks = jax.random.randint(jax.random.fold_in(key, 7), (3, slot_count), 0, 1 << 20)
    first_cell = picks[0] % rows_here
    second_cell = picks[1] % period
    third_cell = picks[2] % period
    return jnp.stack([level_row, radius, first_cell, second_cell, third_cell]).astype(jnp.int32)


def block_levels(key, shape, shards, least, high):
    loudness, own = 1.0, jax.random.fold_in(key, 6)
    for axis_at, parts in shards:
        draws = jnp.exp(jax.random.uniform(jax.random.fold_in(own, axis_at), (parts,), jnp.float32, least / len(shards), high / len(shards)))
        loudness = loudness * jnp.repeat(draws, shape[axis_at] // parts).reshape([-1 if axis == axis_at else 1 for axis in range(len(shape))])
    return loudness


def bell_draw(rng, dims, scale, reach, cuts=(), kind=jnp.bfloat16):
    drawn = jax.random.normal(rng, dims, jnp.float32) * scale
    if len(cuts) > 0:
        drawn = block_levels(rng, dims, cuts, -0.22, 0.18) * drawn
    return jnp.clip(drawn, min=-reach, max=reach).astype(kind)


def setup_inputs(seed: int = 0, part: int = 0) -> dict:
    splits = jax.random.split(jax.random.key(seed), 9)
    own_keys = jax.random.split(jax.random.fold_in(splits[8], part), 9)
    return {
        "fine_cells": draw_fine_cells(jax.random.fold_in(jax.random.fold_in(splits[8], part), 71), part),
        "fine_exponent": jnp.clip(jnp.exp(math.log(0.6) - 2.4849067 * jax.random.uniform(own_keys[1], (FINE,), jnp.float32) ** block_levels(own_keys[1], (FINE,), ((0, 256),), -0.2, 0.2)), 0.05, 0.6),
        "fine_charge": bell_draw(own_keys[2], (FINE,), 1.0, 6.0, ((0, 256),), jnp.float32),
        "fine_offset": jnp.clip(1.0 * jax.random.uniform(own_keys[3], (3, FINE), jnp.float32) ** block_levels(own_keys[3], (3, FINE), ((1, 256),), -0.2, 0.2), 0.0, 1.0),
        "wide_cells": draw_wide_cells(jax.random.fold_in(jax.random.fold_in(splits[8], part), 71), part),
        "wide_exponent": jnp.clip(jnp.exp(math.log(0.6) - 2.4849067 * jax.random.uniform(own_keys[5], (WIDE,), jnp.float32) ** block_levels(own_keys[5], (WIDE,), ((0, 256),), -0.2, 0.2)), 0.05, 0.6),
        "wide_charge": bell_draw(own_keys[6], (WIDE,), 1.0, 6.0, ((0, 256),), jnp.float32),
        "wide_offset": jnp.clip(1.0 * jax.random.uniform(own_keys[7], (3, WIDE), jnp.float32) ** block_levels(own_keys[7], (3, WIDE), ((1, 256),), -0.2, 0.2), 0.0, 1.0),
    }


def one_factor(offsets, radius, exponent, centre_shift):
    inside = jnp.abs(offsets) <= radius[:, None]
    spread = offsets.astype(exponent.dtype) - centre_shift[:, None]
    return jnp.where(inside, jnp.exp(-exponent[:, None] * spread * spread), 0.0)


def deposit(slot_table, exponent, charge, offset, first_level, level_count):
    base_list = []
    grid_cells = 0
    for level_index in range(first_level, first_level + level_count):
        base_list.append(grid_cells)
        grid_cells += (ROWS >> level_index) * (GRID >> level_index) ** 2
    base_table = jnp.array(base_list, dtype=jnp.int32)
    slot_count = slot_table.shape[1]
    batch_size = math.gcd(slot_count, 4096)
    span_cells = jnp.arange(-HALF, HALF + 1, dtype=jnp.int32)
    span_count = 2 * HALF + 1

    def add_batch(flat_grid, batch_index):
        first_slot = (batch_index * batch_size).astype(jnp.int32)
        part_table = lax.dynamic_slice_in_dim(slot_table, first_slot, batch_size, 1)
        part_exponent = lax.dynamic_slice_in_dim(exponent, first_slot, batch_size, 0)
        part_charge = lax.dynamic_slice_in_dim(charge, first_slot, batch_size, 0)
        part_offset = lax.dynamic_slice_in_dim(offset, first_slot, batch_size, 1)
        level_row = part_table[0]
        radius = part_table[1]
        rows_here = jnp.right_shift(jnp.int32(ROWS), level_row)
        period = jnp.right_shift(jnp.int32(GRID), level_row)
        base_cell = base_table[level_row - first_level]
        offsets = jnp.broadcast_to(span_cells[None, :], (batch_size, span_count))
        row_place = part_table[2][:, None] + span_cells[None, :]
        col_place = jnp.mod(part_table[3][:, None] + span_cells[None, :], period[:, None])
        depth_place = jnp.mod(part_table[4][:, None] + span_cells[None, :], period[:, None])
        row_factor = one_factor(offsets, radius, part_exponent, part_offset[0])
        col_factor = one_factor(offsets, radius, part_exponent, part_offset[1])
        depth_factor = one_factor(offsets, radius, part_exponent, part_offset[2])
        plane_weight = ((part_charge[:, None] * row_factor)[:, :, None] * col_factor[:, None, :]).astype(jnp.bfloat16)
        depth_weight = depth_factor.astype(jnp.bfloat16)
        values = plane_weight.astype(jnp.float32)[:, :, :, None] * depth_weight.astype(jnp.float32)[:, None, None, :]
        period_four = period[:, None, None, None]
        flat_index = base_cell[:, None, None, None] + (row_place[:, :, None, None] * period_four + col_place[:, None, :, None]) * period_four + depth_place[:, None, None, :]
        inside_window = (row_place >= 0) & (row_place < rows_here[:, None])
        flat_index = jnp.where(inside_window[:, :, None, None], flat_index, grid_cells).astype(jnp.int32)
        flat_grid = flat_grid.at[flat_index.reshape(-1)].add(values.reshape(-1), mode="drop")
        return flat_grid, None

    start_grid = jnp.zeros((grid_cells,), jnp.float32)
    flat_grid, unused = lax.scan(add_batch, start_grid, jnp.arange(slot_count // batch_size, dtype=jnp.int32))
    return flat_grid


def reference(fine_cells, fine_exponent, fine_charge, fine_offset, wide_cells, wide_exponent, wide_charge, wide_offset):
    fine_flat = deposit(fine_cells, fine_exponent, fine_charge, fine_offset, 0, 2)
    level_zero = ROWS * GRID * GRID
    finest_grid = fine_flat[:level_zero].reshape(ROWS, GRID, GRID)
    second_grid = fine_flat[level_zero:].reshape(ROWS // 2, GRID // 2, GRID // 2)
    wide_flat = deposit(wide_cells, wide_exponent, wide_charge, wide_offset, 2, 3)
    outputs = []
    first_cell = 0
    for level_index in range(2, 5):
        rows_here = ROWS >> level_index
        period = GRID >> level_index
        outputs.append(wide_flat[first_cell:first_cell + rows_here * period * period].reshape(rows_here, period * period))
        first_cell += rows_here * period * period
    return (finest_grid, second_grid, outputs[0], outputs[1], outputs[2])
```

```python
import functools

import jax
import jax.numpy as jnp
from jax import lax
from jax.experimental import pallas as pl
from jax.experimental.pallas import tpu as pltpu
from jax.sharding import PartitionSpec as P

GRID = 512
ROWS = 128
HALF = 4
BLOCK = 256
VALUES = 10
MESH = pl.DeviceIdType.MESH
F32 = jnp.float32
BF16 = jnp.bfloat16


def iota(rows, first=0):
    return lax.broadcasted_iota(jnp.int32, (rows, BLOCK), 0).astype(F32) + float(first)


def band_factor(distance, radius, exponent, shift):
    spread = distance - shift
    return jnp.where(jnp.abs(distance) <= radius, jnp.exp(-exponent * spread * spread), 0.0)


def depth_band(centre, period, radius, exponent, shift):
    start = centre - float(HALF)
    start = jnp.where(start < 0.0, start + period, start)
    tile = jnp.floor(start * 0.0625)
    inner = start - 16.0 * tile + float(HALF)
    following = jnp.where((tile + 1.0) * 16.0 >= period, 0.0, tile + 1.0)
    first = band_factor(iota(16) - inner, radius, exponent, shift).astype(BF16)
    second = band_factor(iota(16, 16) - inner, radius, exponent, shift).astype(BF16)
    return tile, following, first, second


def wide_lanes(row):
    return jnp.broadcast_to(row, (16, BLOCK)).astype(BF16)


def dot_depth(plane, depth):
    return lax.dot_general(plane, depth, (((1,), (1,)), ((), ())), preferred_element_type=F32)


def fine_block(values, brick, column, rows, cols):
    level, radius, c0, c1, c2, exponent, charge, s0, s1, s2 = values
    lower = level < 0.5
    rows_f, cols_f = float(rows), float(cols)
    c0 = c0 - jnp.where(lower, rows_f, rows_f / 2) * brick
    c1 = c1 - jnp.where(lower, cols_f, cols_f / 2) * column
    row_factor = band_factor(iota(rows) - c0, radius, exponent, s0)
    inner = band_factor(iota(cols) - c1, radius, exponent, s1)
    eight = iota(8)
    rim_place = jnp.where(eight < 4.0, eight + jnp.where(lower, cols_f, cols_f / 2), eight - 8.0)
    rim = band_factor(rim_place - c1, radius, exponent, s1)
    first_rows = jnp.where(lower, charge, 0.0) * row_factor
    second_rows = jnp.where(lower, 0.0, charge) * row_factor
    first_cols = jnp.concatenate([inner, rim], 0)
    second_cols = jnp.concatenate([inner[: cols // 2], rim], 0)
    plane = [first_rows[i : i + 1] * first_cols for i in range(rows)]
    plane += [second_rows[i : i + 1] * second_cols for i in range(rows // 2)]
    plane = jnp.concatenate(plane, 0).astype(BF16)
    period = jnp.where(lower, float(GRID), float(GRID // 2))
    tile, following, first, second = depth_band(c2, period, radius, exponent, s2)
    tile, following = wide_lanes(tile), wide_lanes(following)
    zero = jnp.zeros((16, BLOCK), BF16)
    depth = [
        jnp.where(tile == BF16(j), first, jnp.where(following == BF16(j), second, zero))
        for j in range(GRID // 16)
    ]
    return dot_depth(plane, jnp.concatenate(depth, 0))


def wide_block(values, brick, bricks):
    level, radius, c0, c1, c2, exponent, charge, s0, s1, s2 = values
    is_two, is_four = level < 2.5, level > 3.5

    def by_level(two, three, four):
        return jnp.where(is_two, two, jnp.where(is_four, four, three))

    period = by_level(128.0, 64.0, 32.0)
    span = GRID // 4 // bricks
    base = by_level(float(span), span / 2.0, span / 4.0) * brick
    distance = iota(8) + base - c1
    distance = jnp.where(distance < -0.5 * period, distance + period, distance)
    distance = jnp.where(distance >= 0.5 * period, distance - period, distance)
    col_factor = band_factor(distance, radius, exponent, s1)
    row_factor = band_factor(iota(32) - c0, radius, exponent, s0)
    two = by_level(charge, 0.0, 0.0) * row_factor
    three = by_level(0.0, charge, 0.0) * row_factor[:16]
    four = by_level(0.0, 0.0, charge) * row_factor[:8]
    plane = [two * col_factor[i : i + 1] for i in range(span)]
    plane += [three * col_factor[i : i + 1] for i in range(span // 2)]
    plane += [four * col_factor[i : i + 1] for i in range(span // 4)]
    plane = jnp.concatenate(plane, 0).astype(BF16)
    tile, following, first, second = depth_band(c2, period, radius, exponent, s2)
    zero = jnp.zeros((16, BLOCK), BF16)
    depth = []
    for j in range(8):
        here = by_level(float(j), float(j % 4), float(j % 2))
        is_first = wide_lanes(tile - here) == BF16(0)
        is_second = wide_lanes(following - here) == BF16(0)
        depth.append(jnp.where(is_first, first, jnp.where(is_second, second, zero)))
    return dot_depth(plane, jnp.concatenate(depth, 0))


def kernel(
    bricks,
    reps,
    fc_ref,
    fe_ref,
    fq_ref,
    fo_ref,
    wc_ref,
    we_ref,
    wq_ref,
    wo_ref,
    finest_ref,
    second_ref,
    middle_ref,
    coarse_ref,
    coarsest_ref,
    fine_pack,
    wide_pack,
    fine_sum,
    wide_sum,
    right_out,
    left_out,
    right_in,
    left_in,
    right_out2,
    left_out2,
    right_in2,
    left_in2,
    share,
    pair_in,
    paired,
    parts_in,
    mine,
    whole,
    fine_send,
    fine_recv,
    wide_send,
    wide_recv,
    rim_send,
    rim_recv,
    pair_send,
    pair_recv,
    part_send,
    part_recv,
    full_send,
    full_recv,
    last_send,
    last_recv,
):
    group = lax.axis_index("parts")
    brick = lax.axis_index("brick")
    rep = lax.axis_index("rep")
    sub = lax.axis_index("sub")
    column = rep * 2 + sub
    other = 1 - sub
    half = bricks // 2
    rows = finest_ref.shape[0]
    cols = finest_ref.shape[1]

    def at_brick(d):
        return (group, lax.rem(brick + d, bricks), rep, sub)

    def at_rep(d):
        return (group, brick, lax.rem(rep + d, reps), sub)

    partner = (group, brick, rep, other)
    right = (group, brick, lax.rem(rep + sub, reps), other)
    left = (group, brick, lax.rem(rep + sub + reps - 1, reps), other)
    outer = (group, brick, lax.rem(rep + 2 * sub + reps - 1, reps), other)

    barrier = pltpu.get_barrier_semaphore()

    def greet(device):
        pl.semaphore_signal(barrier, inc=1, device_id=device, device_id_type=MESH)

    @pl.loop(1, bricks)
    def _(d):
        greet(at_brick(d))

    @pl.loop(1, reps)
    def _(d):
        greet(at_rep(d))

    greet(partner)
    greet(outer)

    def packed(pack, slot, cells, exponent, charge, offset):
        pack[slot, 0:5, :] = cells[...].astype(F32)
        pack[slot, 5:6, :] = exponent[...]
        pack[slot, 6:7, :] = charge[...]
        pack[slot, 7:10, :] = offset[...]

    packed(wide_pack, 0, wc_ref, we_ref, wq_ref, wo_ref)
    packed(fine_pack, 0, fc_ref, fe_ref, fq_ref, fo_ref)

    fine_sum[...] = jnp.zeros_like(fine_sum)
    wide_sum[...] = jnp.zeros_like(wide_sum)
    brick_f = brick.astype(F32)
    column_f = column.astype(F32)
    blocks = fine_pack.shape[2] // BLOCK

    def fine_from(slot):
        @pl.loop(0, blocks)
        def _(i):
            lanes = pl.ds(pl.multiple_of(i * BLOCK, BLOCK), BLOCK)
            values = [fine_pack[slot, v : v + 1, lanes] for v in range(VALUES)]
            fine_sum[...] += fine_block(values, brick_f, column_f, rows, cols)

    def wide_from(first, second):
        values = [
            jnp.concatenate([wide_pack[first, v : v + 1, :], wide_pack[second, v : v + 1, :]], 1)
            for v in range(VALUES)
        ]
        wide_sum[...] += wide_block(values, brick_f, bricks)

    fine_from(0)

    pl.semaphore_wait(barrier, bricks - 1 + reps - 1 + 2)

    def remote(src, dst, send, recv, device):
        return pltpu.make_async_remote_copy(
            src_ref=src,
            dst_ref=dst,
            send_sem=send,
            recv_sem=recv,
            device_id=device,
            device_id_type=MESH,
        )

    def wide_copy(d):
        return remote(
            wide_pack.at[0], wide_pack.at[d], wide_send.at[d], wide_recv.at[d], at_brick(d)
        )

    def fine_copy(slot):
        device = at_brick(1) if slot == 1 else at_brick(bricks - 1)
        return remote(
            fine_pack.at[0], fine_pack.at[slot], fine_send.at[slot], fine_recv.at[slot], device
        )

    wide_copy(half).start()

    @pl.loop(1, half)
    def _(i):
        wide_copy(half - i).start()
        wide_copy(half + i).start()

    fine_copy(1).start()
    fine_copy(2).start()

    for slot in (1, 2):
        fine_copy(slot).wait_recv()
        fine_from(slot)

    span = cols + 8
    for i in range(rows):
        at = i * span + cols
        right_out[4 * i : 4 * i + 4, :] = fine_sum[at : at + 4, :]
        left_out[4 * i : 4 * i + 4, :] = fine_sum[at + 4 : at + 8, :]
    span2 = cols // 2 + 8
    depth2 = second_ref.shape[2]
    for i in range(rows // 2):
        at = rows * span + i * span2 + cols // 2
        right_out2[4 * i : 4 * i + 4, :] = fine_sum[at : at + 4, :depth2]
        left_out2[4 * i : 4 * i + 4, :] = fine_sum[at + 4 : at + 8, :depth2]
    rims = [
        remote(right_out, left_in, rim_send.at[0], rim_recv.at[0], right),
        remote(left_out, right_in, rim_send.at[1], rim_recv.at[1], left),
        remote(right_out2, left_in2, rim_send.at[2], rim_recv.at[2], right),
        remote(left_out2, right_in2, rim_send.at[3], rim_recv.at[3], left),
    ]
    for copy in rims:
        copy.start()

    @pl.loop(1, half)
    def _(i):
        wide_copy(i).wait_recv()
        wide_copy(bricks - i).wait_recv()
        wide_from(i, bricks - i)

    wide_copy(half).wait_recv()
    wide_from(0, half)

    for p in range(16):
        share[p, 0:16, :] = wide_sum[16 * p : 16 * p + 16, :]
    lane = lax.broadcasted_iota(jnp.int32, (8, 128), 1)
    for pair in range(2):
        for h in range(2):
            at = 256 + pair * 32 + 8 * h
            share[2 * pair + h, 16:24, :] = jnp.where(
                lane < 64, wide_sum[at : at + 8, :], wide_sum[at + 16 : at + 24, :]
            )
    share[4, 16:24, :] = jnp.where(lane < 32, wide_sum[320:328, :], wide_sum[328:336, :])
    for p in range(5, 16):
        share[p, 16:24, :] = jnp.zeros((8, 128), F32)

    pair_copy = remote(share.at[pl.ds(other * 8, 8)], pair_in, pair_send, pair_recv, partner)
    pair_copy.start()
    pair_copy.wait_recv()
    paired[...] = share[pl.ds(sub * 8, 8)] + pair_in[...]

    def part_copy(d):
        return remote(
            paired.at[lax.rem(rep + d, reps)],
            parts_in.at[d],
            part_send.at[d],
            part_recv.at[d],
            at_rep(d),
        )

    @pl.loop(1, reps)
    def _(d):
        part_copy(d).start()

    for copy in rims:
        copy.wait_recv()
    for i in range(rows):
        at = i * span
        finest_ref[i, :, :] = fine_sum[at : at + cols, :]
        finest_ref[i, 0:4, :] += left_in[4 * i : 4 * i + 4, :]
        finest_ref[i, cols - 4 : cols, :] += right_in[4 * i : 4 * i + 4, :]
    for i in range(rows // 2):
        at = rows * span + i * span2
        second_ref[i, :, :] = fine_sum[at : at + cols // 2, :depth2]
        second_ref[i, 0:4, :] += left_in2[4 * i : 4 * i + 4, :]
        second_ref[i, cols // 2 - 4 : cols // 2, :] += right_in2[4 * i : 4 * i + 4, :]

    total = paired[rep]
    for d in range(1, reps):
        part_copy(d).wait_recv()
        total = total + parts_in[d]
    mine[...] = total
    slot = sub * 8 + rep
    whole[slot] = total

    def full_copy(d, to):
        return remote(mine, whole.at[to], full_send.at[d], full_recv.at[d], at_rep(d))

    @pl.loop(1, reps)
    def _(d):
        full_copy(d, slot).start()

    @pl.loop(1, reps)
    def _(d):
        full_copy(d, sub * 8 + lax.rem(rep + reps - d, reps)).wait_recv()

    last = remote(
        whole.at[pl.ds(sub * 8, 8)], whole.at[pl.ds(sub * 8, 8)], last_send, last_recv, partner
    )
    last.start()
    last_in = remote(
        whole.at[pl.ds(sub * 8, 8)], whole.at[pl.ds(other * 8, 8)], last_send, last_recv, partner
    )
    last_in.wait_recv()

    for c in range(8):
        for h in range(4):
            t = 4 * c + h
            middle_ref[8 * h : 8 * h + 8, 128 * c : 128 * c + 128] = whole[
                t // 2, 8 * (t % 2) : 8 * (t % 2) + 8, :
            ]
    for pair in range(2):
        for h in range(2):
            coarse_ref[8 * h : 8 * h + 8, 128 * pair : 128 * pair + 128] = whole[
                2 * pair + h, 16:24, :
            ]
    coarsest_ref[...] = whole[4, 16:24, :64]

    @pl.loop(1, bricks)
    def _(d):
        wide_copy(d).wait_send()

    for slot in (1, 2):
        fine_copy(slot).wait_send()
    for copy in rims:
        copy.wait_send()
    pair_copy.wait_send()

    @pl.loop(1, reps)
    def _(d):
        part_copy(d).wait_send()
        full_copy(d, sub * 8 + rep).wait_send()

    last.wait_send()


def per_device(bricks, reps, fc, fe, fq, fo, wc, we, wq, wo):
    columns = reps * 2
    rows, cols = ROWS // bricks, GRID // columns
    fine, wide = fe.shape[0], we.shape[0]
    share = (GRID // 4) ** 2 // bricks
    vmem = pl.BlockSpec(memory_space=pltpu.VMEM)
    dma = pltpu.SemaphoreType.DMA
    tall = rows * (cols + 8) + rows // 2 * (cols // 2 + 8)
    rim, rim2 = (rows * 4, GRID), (rows * 2, GRID // 2)
    return pl.pallas_call(
        functools.partial(kernel, bricks, reps),
        out_shape=(
            jax.ShapeDtypeStruct((rows, cols, GRID), F32),
            jax.ShapeDtypeStruct((rows // 2, cols // 2, GRID // 2), F32),
            jax.ShapeDtypeStruct((ROWS // 4, share), F32),
            jax.ShapeDtypeStruct((ROWS // 8, share // 4), F32),
            jax.ShapeDtypeStruct((ROWS // 16, share // 16), F32),
        ),
        in_specs=[vmem] * 8,
        out_specs=(vmem,) * 5,
        scratch_shapes=[
            pltpu.VMEM((3, VALUES, fine), F32),
            pltpu.VMEM((bricks, VALUES, wide), F32),
            pltpu.VMEM((tall, GRID), F32),
            pltpu.VMEM((336, 128), F32),
            *[pltpu.VMEM(rim, F32) for _ in range(4)],
            *[pltpu.VMEM(rim2, F32) for _ in range(4)],
            pltpu.VMEM((16, 24, 128), F32),
            pltpu.VMEM((8, 24, 128), F32),
            pltpu.VMEM((8, 24, 128), F32),
            pltpu.VMEM((8, 24, 128), F32),
            pltpu.VMEM((24, 128), F32),
            pltpu.VMEM((16, 24, 128), F32),
            dma((3,)),
            dma((3,)),
            dma((bricks,)),
            dma((bricks,)),
            dma((4,)),
            dma((4,)),
            dma,
            dma,
            dma((reps,)),
            dma((reps,)),
            dma((reps,)),
            dma((reps,)),
            dma,
            dma,
        ],
        compiler_params=pltpu.CompilerParams(collective_id=0, has_side_effects=True),
    )(
        fc,
        fe.reshape(1, fine),
        fq.reshape(1, fine),
        fo,
        wc,
        we.reshape(1, wide),
        wq.reshape(1, wide),
        wo,
    )


def solution(mesh):
    everyone = ("parts", "brick", "rep", "sub")
    return jax.shard_map(
        functools.partial(per_device, mesh.shape["brick"], mesh.shape["rep"]),
        mesh=mesh,
        in_specs=(
            P(None, everyone),
            P(everyone),
            P(everyone),
            P(None, everyone),
            P(None, everyone),
            P(everyone),
            P(everyone),
            P(None, everyone),
        ),
        out_specs=(
            P(("parts", "brick"), ("rep", "sub"), None),
            P(("parts", "brick"), ("rep", "sub"), None),
            P("parts", "brick"),
            P("parts", "brick"),
            P("parts", "brick"),
        ),
        check_vma=False,
    )
```
